32 devices in a mesh: dp: 2 (over x), sp: 16 (over y, z, core).
Axes of the slice: x: 2, y: 2, z: 4, core: 2. Of those that a mesh axis runs over, the one named last changes fastest.
Arguments:
- x: bfloat16 [4096, 8192], P(('dp', 'sp')), parts along dimension 0
- gain: bfloat16 [8192], replicated
- wq: bfloat16 [8192, 8192], replicated
- wk: bfloat16 [8192, 8192], replicated
- wv: bfloat16 [8192, 8192], replicated
- wo: bfloat16 [8192, 8192], replicated
Outputs:
- output: bfloat16 [4096, 8192], P(('dp', 'sp')), parts along dimension 0
There are 2 independent parts. The reference program is written for one: setup_inputs(seed, part) draws one part's arguments, and reference() takes and returns one part's arrays. A program takes and returns all parts, laid end to end along the dimension named above; an argument that names none is the same for every part.
All inputs are finite; a program needn't handle non-finite values.
Results may differ from the reference program's by a relative error of at most 0.012.
Values are sent between devices in bfloat16 or wider.
A program may use at most 2 GiB of HBM per device.

```python
import jax
import jax.numpy as jnp
from jax import lax

ROWS = 2048
D = 8192
HEADS = 64
KV_HEADS = 64
HEAD = 128
THETA = 10000


def setup_inputs(seed: int = 0, part: int = 0) -> dict:
    kx, kn, kq, kk, kv, ko = jax.random.split(jax.random.key(seed), 6)

    def weights(key, rows, columns):
        return jax.random.normal(key, (rows, columns), jnp.float32) * rows**-0.5

    drawn = {
        "x": jax.random.normal(jax.random.fold_in(kx, part), (ROWS, D), jnp.float32),
        "gain": 1 + 0.1 * jax.random.normal(kn, (D,), jnp.float32),
        "wq": 2 * weights(kq, D, HEADS * HEAD),
        "wk": 2 * weights(kk, D, KV_HEADS * HEAD),
        "wv": 4 * weights(kv, D, KV_HEADS * HEAD),
        "wo": weights(ko, HEADS * HEAD, D),
    }
    return {k: v.astype(jnp.bfloat16) for k, v in drawn.items()}


def normed(x, gain):
    wide = x.astype(jnp.float32)
    scale = lax.rsqrt(jnp.mean(wide * wide, -1, keepdims=True) + 1e-6)
    return (wide * scale * gain.astype(jnp.float32)).astype(jnp.bfloat16)


def turned(t, place, theta):
    half = t.shape[-1] // 2
    angle = place.astype(jnp.float32)[:, None] * theta ** (-jnp.arange(half, dtype=jnp.float32) / half)
    cos, sin = jnp.cos(angle)[:, None], jnp.sin(angle)[:, None]
    a, b = t[..., :half].astype(jnp.float32), t[..., half:].astype(jnp.float32)
    return jnp.concatenate([a * cos - b * sin, b * cos + a * sin], -1).astype(jnp.bfloat16)


def matmul(a, w):
    return jnp.dot(a, w, preferred_element_type=jnp.float32).astype(jnp.bfloat16)


def einsum(form, a, b):
    return jnp.einsum(form, a.astype(jnp.float32), b.astype(jnp.float32))


def attention(q, k, v):
    scores = einsum("tgsd,ugd->gstu", q, k) * q.shape[-1] ** -0.5
    token = jnp.arange(q.shape[0])
    scores = jnp.where(token[:, None] >= token, scores, -jnp.inf)
    weights = jax.nn.softmax(scores, -1).astype(jnp.bfloat16)
    return einsum("gstu,ugd->tgsd", weights, v).astype(jnp.bfloat16)


def reference(x, gain, wq, wk, wv, wo):
    a, place = normed(x, gain), jnp.arange(ROWS)
    q = turned(matmul(a, wq).reshape(ROWS, HEADS, HEAD), place, THETA).reshape(ROWS, KV_HEADS, -1, HEAD)
    k = turned(matmul(a, wk).reshape(ROWS, KV_HEADS, HEAD), place, THETA)
    v = matmul(a, wv).reshape(ROWS, KV_HEADS, HEAD)
    seen = attention(q, k, v).reshape(ROWS, HEADS * HEAD)
    return (x.astype(jnp.float32) + jnp.dot(seen, wo, preferred_element_type=jnp.float32)).astype(jnp.bfloat16)
```

```python
import functools

import jax
import jax.numpy as jnp
from jax import lax
from jax.experimental import pallas as pl
from jax.experimental.pallas import tpu as pltpu
from jax.sharding import PartitionSpec as P

HEAD = 128
THETA = 10000
LOG2E = 1.4426950408889634
NEG = -1e30
MESH = pl.DeviceIdType.MESH
TILE = 256


def normed(x, gain):
    wide = x.astype(jnp.float32)
    scale = lax.rsqrt(jnp.mean(wide * wide, -1, keepdims=True) + 1e-6)
    return (wide * scale * gain.astype(jnp.float32)).astype(jnp.bfloat16)


def _dot(a, b, ca, cb):
    return lax.dot_general(a, b, (((ca,), (cb,)), ((), ())), preferred_element_type=jnp.float32)


def _kernel(chips, a_ref, x_ref, cos_ref, sin_ref, wq, wk, wv, wo, y_ref, a_v, x_v, send, recv, osend, orecv, part, vt_s,
            load_sem, pair_send, pair_recv, q_send, q_recv, o_send, o_recv, p_send, p_recv):
    own, d = a_ref.shape
    rows = 2 * own
    tokens = chips * rows
    waves = recv.shape[0] // 3
    per = 3 * chips
    half = waves * chips * TILE
    steps = waves * per
    me = lax.axis_index("sp")
    core, chip = lax.rem(me, 2), lax.div(me, 2)
    other = 1 - core
    partner = {"sp": 2 * chip + other}
    at = lambda c: {"sp": 2 * c + core}
    near = lambda o: lax.rem(chip + 1 + o, chips)
    mine = pl.ds(pl.multiple_of(own * core, own), own)
    theirs = pl.ds(pl.multiple_of(own * other, own), own)
    block = lambda c: pl.ds(pl.multiple_of(rows * c, rows), rows)

    load_a = pltpu.make_async_copy(a_ref, a_v.at[mine], load_sem.at[0])
    load_x = pltpu.make_async_copy(x_ref, x_v, load_sem.at[1])
    load_a.start()
    load_x.start()

    barrier = pltpu.get_barrier_semaphore()
    pl.semaphore_signal(barrier, inc=1, device_id=partner, device_id_type=MESH)

    def greet(o, _):
        pl.semaphore_signal(barrier, inc=1, device_id=at(near(o)), device_id_type=MESH)

    def project(slots, slot_sem):
        def fetch(i):
            w, t, o = lax.div(i, per), lax.rem(lax.div(i, chips), 3), lax.rem(i, chips)
            column = pl.multiple_of(half * core + (w * chips + near(o)) * TILE, TILE)
            slot = lax.rem(i, 3)
            for n, ref in enumerate((wq, wk, wv)):

                @pl.when(t == n)
                def _():
                    pltpu.make_async_copy(ref.at[:, pl.ds(column, TILE)], slots.at[slot], slot_sem.at[slot]).start()

        def out_copy(i):
            g, o = lax.div(i, chips), lax.rem(i, chips)
            n = g * (chips - 1) + o
            return pltpu.make_async_remote_copy(send.at[n], recv.at[g, block(chip)], q_send.at[n], q_recv.at[g, chip],
                                                device_id=at(near(o)), device_id_type=MESH)

        fetch(jnp.int32(0))
        fetch(jnp.int32(1))
        lax.fori_loop(0, chips - 1, greet, None)
        pl.semaphore_wait(barrier, chips)
        share = pltpu.make_async_remote_copy(a_ref, a_v.at[mine], pair_send, pair_recv, device_id=partner, device_id_type=MESH)
        share.start()
        load_a.wait()
        share.wait()

        def step(i, _):
            g, o = lax.div(i, chips), lax.rem(i, chips)
            t = lax.rem(g, 3)
            slot = lax.rem(i, 3)
            pltpu.make_async_copy(wq.at[:, pl.ds(0, TILE)], slots.at[slot], slot_sem.at[slot]).wait()

            @pl.when(i + 2 < steps)
            def _():
                fetch(i + 2)

            got = _dot(a_v[...], slots[slot], 1, 0).astype(jnp.bfloat16)

            def store(value, cols):
                @pl.when(o < chips - 1)
                def _():
                    send[g * (chips - 1) + o, :, cols] = value

                @pl.when(o == chips - 1)
                def _():
                    recv[g, block(chip), cols] = value

            for h in range(TILE // HEAD):
                cols = slice(h * HEAD, (h + 1) * HEAD)

                @pl.when(t < 2)
                def _():
                    wide = got[:, cols].astype(jnp.float32)
                    store((wide * cos_ref[...] + pltpu.roll(wide, HEAD // 2, 1) * sin_ref[...]).astype(jnp.bfloat16), cols)

                @pl.when(t == 2)
                def _():
                    store(got[:, cols], cols)

            @pl.when(o > 0)
            def _():
                out_copy(i - 1).start()

        lax.fori_loop(0, steps, step, None)

    pl.run_scoped(project, pltpu.VMEM((3, d, TILE), jnp.bfloat16), pltpu.SemaphoreType.DMA((3,)))

    def finish(slots, acc, slot_sem):
        chunks = waves * chips

        def source(n):
            return lax.div(n, chips), lax.rem(chip + chips - lax.rem(n, chips), chips)

        def fetch(n):
            w, c = source(n)
            row = pl.multiple_of(half * core + (w * chips + c) * TILE, TILE)
            slot = lax.rem(n, 4)
            pltpu.make_async_copy(wo.at[pl.ds(row, TILE), :], slots.at[slot], slot_sem.at[slot]).start()

        for n in range(3):
            fetch(jnp.int32(n))

        strip = 512
        hidden = lax.broadcasted_iota(jnp.int32, (strip, strip), 0) > lax.broadcasted_iota(jnp.int32, (strip, strip), 1)
        e = HEAD**-0.5 * LOG2E

        def attend(w, _):
            def arrived(n, _):
                t, c = lax.div(n, chips - 1), near(lax.rem(n, chips - 1))
                g = 3 * w + t
                pltpu.make_async_remote_copy(send.at[0], recv.at[g, block(c)], q_send.at[0], q_recv.at[g, c],
                                             device_id=at(c), device_id_type=MESH).wait_recv()

            lax.fori_loop(0, 3 * (chips - 1), arrived, None)
            for h in range(2):
                vt_s[h, :HEAD, :] = recv[3 * w + 2, :, h * HEAD : (h + 1) * HEAD].T
                vt_s[h, HEAD:, :] = jnp.ones((16, tokens), jnp.bfloat16)
            for i in range(tokens // strip):

                def head(h, _):
                    lanes = pl.ds(pl.multiple_of(h * HEAD, HEAD), HEAD)
                    q = recv[3 * w, i * strip : (i + 1) * strip, lanes]
                    scores = [_dot(recv[3 * w + 1, b * strip : (b + 1) * strip, lanes], q, 1, 1) for b in range(i + 1)]
                    scores[i] = jnp.where(hidden, NEG, scores[i])
                    top = functools.reduce(jnp.maximum, [s.max(axis=0, keepdims=True) for s in scores])
                    mix = 0
                    for b, s in enumerate(scores):
                        weights = jnp.exp2((s - top) * e).astype(jnp.bfloat16)
                        mix = mix + _dot(vt_s[h, :, b * strip : (b + 1) * strip], weights, 1, 0)
                    seen = (mix[:HEAD] * (1 / mix[HEAD : HEAD + 1])).T.astype(jnp.bfloat16)
                    osend[w, i * strip : (i + 1) * strip, lanes] = seen

                lax.fori_loop(0, 2, head, None)
            orecv[w, chip] = osend[w, block(chip)]

            def give(o, _):
                c = near(o)
                pltpu.make_async_remote_copy(osend.at[w, block(c)], orecv.at[w, chip], o_send.at[w, o], o_recv.at[w, chip],
                                             device_id=at(c), device_id_type=MESH).start()

            lax.fori_loop(0, chips - 1, give, None)

        lax.fori_loop(0, waves, attend, None)

        piece = part.shape[2]
        pieces = d // piece
        across = lambda n: pl.ds(pl.multiple_of(n * piece, piece), piece)

        def hand(n):
            return pltpu.make_async_remote_copy(acc.at[n, theirs], part.at[n], p_send.at[n], p_recv.at[n],
                                                device_id=partner, device_id_type=MESH)

        def chunk(n, _):
            w, c = source(n)
            slot = lax.rem(n, 4)

            @pl.when(n + 3 < chunks)
            def _():
                fetch(n + 3)

            @pl.when(c != chip)
            def _():
                pltpu.make_async_remote_copy(osend.at[w, block(c)], orecv.at[w, c], o_send.at[w, 0], o_recv.at[w, c],
                                             device_id=at(c), device_id_type=MESH).wait_recv()

            pltpu.make_async_copy(wo.at[pl.ds(0, TILE), :], slots.at[slot], slot_sem.at[slot]).wait()
            seen = orecv[w, c]

            def columns(p, _):
                more = _dot(seen, slots[slot, :, across(p)], 1, 0)

                @pl.when(n == 0)
                def _():
                    acc[p] = more

                @pl.when(n > 0)
                def _():
                    acc[p] += more

                @pl.when((n == chunks - 1) & (p > 0))
                def _():
                    hand(p - 1).start()

            lax.fori_loop(0, pieces, columns, None)

        lax.fori_loop(0, chunks, chunk, None)
        load_x.wait()
        hand(pieces - 1).start()

        def add(n, _):
            hand(n).wait_recv()
            total = acc[n, mine, :] + part[n]
            y_ref[:, across(n)] = (x_v[:, across(n)].astype(jnp.float32) + total).astype(jnp.bfloat16)
            hand(n).wait_send()

        lax.fori_loop(0, pieces, add, None)

        def sent(n, _):
            g, o = lax.div(n, chips - 1), lax.rem(n, chips - 1)
            pltpu.make_async_remote_copy(send.at[n], recv.at[g, block(chip)], q_send.at[n], q_recv.at[g, chip],
                                         device_id=at(near(o)), device_id_type=MESH).wait_send()

        lax.fori_loop(0, 3 * waves * (chips - 1), sent, None)

        def given(n, _):
            w, o = lax.div(n, chips - 1), lax.rem(n, chips - 1)
            c = near(o)
            pltpu.make_async_remote_copy(osend.at[w, block(c)], orecv.at[w, chip], o_send.at[w, o], o_recv.at[w, chip],
                                         device_id=at(c), device_id_type=MESH).wait_send()

        lax.fori_loop(0, waves * (chips - 1), given, None)

    pl.run_scoped(finish, pltpu.VMEM((4, TILE, d), jnp.bfloat16), pltpu.VMEM((d // part.shape[2], rows, part.shape[2]), jnp.float32),
                  pltpu.SemaphoreType.DMA((4,)))


def solution(mesh):
    chips = mesh.shape["sp"] // 2

    def step(x, gain, wq, wk, wv, wo):
        own, d = x.shape
        rows, tokens = 2 * own, 2 * own * chips
        waves = wq.shape[1] // (2 * chips * TILE)
        piece = 1024
        a = normed(x, gain)
        place = lax.div(lax.axis_index("sp"), 2) * rows + jnp.arange(rows)
        turn = HEAD // 2
        angle = place.astype(jnp.float32)[:, None] * THETA ** (-jnp.arange(turn, dtype=jnp.float32) / turn)
        cos, sin = jnp.cos(angle), jnp.sin(angle)
        cos, sin = jnp.concatenate([cos, cos], -1), jnp.concatenate([-sin, sin], -1)
        hbm, vmem = pl.BlockSpec(memory_space=pl.ANY), pl.BlockSpec(memory_space=pltpu.VMEM)
        dma, low = pltpu.SemaphoreType.DMA, jnp.bfloat16
        return pl.pallas_call(
            functools.partial(_kernel, chips),
            out_shape=jax.ShapeDtypeStruct((own, d), low),
            in_specs=[hbm, hbm, vmem, vmem, hbm, hbm, hbm, hbm],
            out_specs=vmem,
            scratch_shapes=[
                pltpu.VMEM((rows, d), low),
                pltpu.VMEM((own, d), low),
                pltpu.VMEM((3 * waves * (chips - 1), rows, TILE), low),
                pltpu.VMEM((3 * waves, tokens, TILE), low),
                pltpu.VMEM((waves, tokens, TILE), low),
                pltpu.VMEM((waves, chips, rows, TILE), low),
                pltpu.VMEM((d // piece, own, piece), jnp.float32),
                pltpu.VMEM((2, HEAD + 16, tokens), low),
                dma((2,)),
                dma,
                dma,
                dma((3 * waves * (chips - 1),)),
                dma((3 * waves, chips)),
                dma((waves, chips - 1)),
                dma((waves, chips)),
                dma((d // piece,)),
                dma((d // piece,)),
            ],
            compiler_params=pltpu.CompilerParams(collective_id=0, has_side_effects=True, vmem_limit_bytes=67043328),
        )(a, x, cos, sin, wq, wk, wv, wo)

    rows, whole = P(("dp", "sp"), None), P(None, None)
    return jax.shard_map(
        step,
        mesh=mesh,
        in_specs=(rows, P(None), whole, whole, whole, whole),
        out_specs=rows,
        check_vma=False,
    )
```

```python
import functools

import jax
import jax.numpy as jnp
import numpy as np
from jax import lax
from jax.experimental import pallas as pl
from jax.experimental.pallas import tpu as pltpu
from jax.sharding import PartitionSpec as P

HEAD = 128
THETA = 10000
LOG2E = 1.4426950408889634
NEG = -1e30
MESH = pl.DeviceIdType.MESH
TILE = 256
CHIPS, SIDE = 8, 4


def _dot(a, b, ca, cb):
    return lax.dot_general(a, b, (((ca,), (cb,)), ((), ())), preferred_element_type=jnp.float32)


def _kernel(x_ref, gain_ref, turn_ref, wq, wk, wv, wo, y_ref, a_v, x_v, turn_v, cos_v, sin_v, send, lend, recv, osend, orecv, part, vt_s,
            load_sem, pair_send, pair_recv, lent_send, lent_recv, pass_send, pass_recv, c_send, l_send, q_recv, o_send, o_recv,
            p_send, p_recv):
    own, d = x_ref.shape
    rows = 2 * own
    tokens = CHIPS * rows
    waves = recv.shape[0] // 3
    groups = 3 * waves
    phase = groups * SIDE
    half = waves * CHIPS * TILE
    me = lax.axis_index("sp")
    core, chip = lax.rem(me, 2), lax.div(me, 2)
    side = lax.rem(lax.div(chip, 2), 2)
    place = lax.div(chip, SIDE) * 2 + lax.rem(chip, 2)
    other = 1 - core
    partner = {"sp": 2 * chip + other}
    at = lambda c: {"sp": 2 * c + core}
    chip_of = lambda s, m: lax.div(m, 2) * SIDE + s * 2 + lax.rem(m, 2)
    near = lambda o: lax.rem(place + 1 + o, SIDE)
    counter = chip_of(1 - side, place)
    mine = pl.ds(pl.multiple_of(own * core, own), own)
    theirs = pl.ds(pl.multiple_of(own * other, own), own)
    block = lambda c: pl.ds(pl.multiple_of(rows * c, rows), rows)
    first = lambda c: pl.ds(pl.multiple_of(rows * c, own), own)
    second = lambda c: pl.ds(pl.multiple_of(rows * c + own, own), own)
    bit = own // 2
    lent = lambda k: pl.ds(pl.multiple_of(bit * k, bit), bit)
    borrowed = lambda k: pl.ds(pl.multiple_of(rows + bit * k, bit), bit)

    load_x = pltpu.make_async_copy(x_ref, x_v, load_sem.at[0])
    load_turn = pltpu.make_async_copy(turn_ref.at[block(chip)], turn_v.at[pl.ds(0, rows)], load_sem.at[1])
    load_more = pltpu.make_async_copy(turn_ref.at[first(counter)], turn_v.at[pl.ds(rows, own)], load_sem.at[2])
    load_x.start()
    load_turn.start()
    load_more.start()

    barrier = pltpu.get_barrier_semaphore()
    pl.semaphore_signal(barrier, inc=1, device_id=partner, device_id_type=MESH)

    def greet(o, _):
        pl.semaphore_signal(barrier, inc=1, device_id=at(lax.rem(chip + 1 + o, CHIPS)), device_id_type=MESH)

    lax.fori_loop(0, CHIPS - 1, greet, None)

    def cross_copy(r):
        g, o = lax.div(r, SIDE), lax.rem(r, SIDE)
        return pltpu.make_async_remote_copy(send.at[r], recv.at[g, second(chip)], c_send.at[r], q_recv.at[g, place, 2],
                                            device_id=at(chip_of(1 - side, near(o))), device_id_type=MESH)

    def own_copies(n):
        g, o = lax.div(n, SIDE - 1), lax.rem(n, SIDE - 1)
        to = at(chip_of(side, near(o)))
        return (
            pltpu.make_async_remote_copy(lend.at[n, pl.ds(0, rows)], recv.at[g, block(chip)], l_send.at[n, 0], q_recv.at[g, place, 0],
                                         device_id=to, device_id_type=MESH),
            pltpu.make_async_remote_copy(lend.at[n, pl.ds(rows, own)], recv.at[g, first(counter)], l_send.at[n, 1],
                                         q_recv.at[g, place, 1], device_id=to, device_id_type=MESH),
        )

    def project(slots, slot_sem):
        def fetch(i):
            s, r = lax.div(i, phase), lax.rem(i, phase)
            g, o = lax.div(r, SIDE), lax.rem(r, SIDE)
            w, t = lax.div(g, 3), lax.rem(g, 3)
            to = chip_of(lax.rem(side + 1 + s, 2), near(o))
            column = pl.multiple_of(half * core + (w * CHIPS + to) * TILE, TILE)
            slot = lax.rem(i, 3)
            for n, ref in enumerate((wq, wk, wv)):

                @pl.when(t == n)
                def _():
                    pltpu.make_async_copy(ref.at[:, pl.ds(column, TILE)], slots.at[slot], slot_sem.at[slot]).start()

        fetch(jnp.int32(0))
        fetch(jnp.int32(1))
        load_x.wait()

        def norm(n, _):
            span = pl.ds(pl.multiple_of(n * 16, 16), 16)
            wide = x_v[span, :].astype(jnp.float32)
            scale = lax.rsqrt(jnp.mean(wide * wide, -1, keepdims=True) + 1e-6)
            a_v[pl.ds(pl.multiple_of(own * core + n * 16, 16), 16), :] = (wide * scale * gain_ref[...].astype(jnp.float32)).astype(jnp.bfloat16)

        lax.fori_loop(0, own // 16, norm, None)
        load_turn.wait()
        load_more.wait()
        low = lax.broadcasted_iota(jnp.int32, (rows + own, HEAD), 1) < HEAD // 2
        here = turn_v[...]
        there = pltpu.roll(here, HEAD // 2, 1)
        cos_v[...] = jnp.where(low, here, there)
        sin_v[...] = jnp.where(low, -there, here)
        pl.semaphore_wait(barrier, CHIPS)
        share = pltpu.make_async_remote_copy(a_v.at[mine], a_v.at[mine], pair_send, pair_recv, device_id=partner, device_id_type=MESH)
        share.start()
        share.wait()
        lending = pltpu.make_async_remote_copy(a_v.at[lent(core)], a_v.at[borrowed(core)], lent_send, lent_recv,
                                               device_id=at(counter), device_id_type=MESH)
        lending.start()

        def tile(i, high, low, store):
            slot = lax.rem(i, 3)
            t = lax.rem(lax.div(i, SIDE), 3)
            pltpu.make_async_copy(wq.at[:, pl.ds(0, TILE)], slots.at[slot], slot_sem.at[slot]).wait()

            @pl.when(i + 2 < 2 * phase)
            def _():
                fetch(i + 2)

            got = _dot(a_v[low:high, :], slots[slot], 1, 0).astype(jnp.bfloat16)
            for h in range(TILE // HEAD):
                cols = slice(h * HEAD, (h + 1) * HEAD)

                @pl.when(t < 2)
                def _():
                    wide = got[:, cols].astype(jnp.float32)
                    turned = wide * cos_v[low:high, :] + pltpu.roll(wide, HEAD // 2, 1) * sin_v[low:high, :]
                    store(turned.astype(jnp.bfloat16), cols)

                @pl.when(t == 2)
                def _():
                    store(got[:, cols], cols)

        def cross(r, _):
            def store(value, cols):
                send[r, :, cols] = value

            tile(r, rows, own, store)

            @pl.when(r > 0)
            def _():
                cross_copy(r - 1).start()

        lax.fori_loop(0, phase, cross, None)
        lending.wait_recv()
        passing = pltpu.make_async_remote_copy(a_v.at[borrowed(core)], a_v.at[borrowed(core)], pass_send, pass_recv,
                                               device_id=partner, device_id_type=MESH)
        passing.start()
        cross_copy(phase - 1).start()
        passing.wait()
        lending.wait_send()

        def within(r, _):
            g, o = lax.div(r, SIDE), lax.rem(r, SIDE)
            n = g * (SIDE - 1) + o

            def store(value, cols):
                @pl.when(o < SIDE - 1)
                def _():
                    lend[n, :, cols] = value

                @pl.when(o == SIDE - 1)
                def _():
                    recv[g, block(chip), cols] = value[:rows]
                    recv[g, first(counter), cols] = value[rows:]

            tile(phase + r, rows + own, 0, store)

            @pl.when(o > 0)
            def _():
                for copy in own_copies(n - 1):
                    copy.start()

        lax.fori_loop(0, phase, within, None)

    pl.run_scoped(project, pltpu.VMEM((3, d, TILE), jnp.bfloat16), pltpu.SemaphoreType.DMA((3,)))

    def give_copy(w, s, o):
        c = chip_of(lax.rem(side + 1 + s, 2), near(o))
        return pltpu.make_async_remote_copy(osend.at[w, block(c)], orecv.at[w, lax.rem(1 + s, 2), place], o_send.at[w, s, o],
                                            o_recv.at[w, lax.rem(1 + s, 2), place], device_id=at(c), device_id_type=MESH)

    def finish(slots, acc, slot_sem):
        parts, wide = acc.shape[0], acc.shape[2]
        chunks = waves * 2 * parts

        def fetch(n):
            w, far, p = lax.div(n, 2 * parts), lax.rem(lax.div(n, parts), 2), lax.rem(n, parts)
            slot = lax.rem(n, 3)
            across = pl.ds(pl.multiple_of(p * wide, wide), wide)

            def source(m, _):
                row = pl.multiple_of(half * core + (w * CHIPS + chip_of(lax.rem(side + far, 2), m)) * TILE, TILE)
                into = pl.ds(pl.multiple_of(m * TILE, TILE), TILE)
                pltpu.make_async_copy(wo.at[pl.ds(row, TILE), across], slots.at[slot, into], slot_sem.at[slot]).start()

            lax.fori_loop(0, SIDE, source, None)

        fetch(jnp.int32(0))
        fetch(jnp.int32(1))

        strip = 512
        hidden = lax.broadcasted_iota(jnp.int32, (strip, strip), 0) > lax.broadcasted_iota(jnp.int32, (strip, strip), 1)
        e = HEAD**-0.5 * LOG2E

        def attend(w, _):
            def arrived(n, _):
                g, o = 3 * w + lax.div(n, SIDE), lax.rem(n, SIDE)
                m = near(o)

                @pl.when(o < SIDE - 1)
                def _():
                    c = chip_of(side, m)
                    pltpu.make_async_remote_copy(lend.at[0, pl.ds(0, rows)], recv.at[g, block(c)], l_send.at[0, 0], q_recv.at[g, m, 0],
                                                 device_id=at(c), device_id_type=MESH).wait_recv()
                    pltpu.make_async_remote_copy(lend.at[0, pl.ds(rows, own)], recv.at[g, first(chip_of(1 - side, m))], l_send.at[0, 1],
                                                 q_recv.at[g, m, 1], device_id=at(c), device_id_type=MESH).wait_recv()

                c = chip_of(1 - side, m)
                pltpu.make_async_remote_copy(send.at[0], recv.at[g, second(c)], c_send.at[0], q_recv.at[g, m, 2],
                                             device_id=at(c), device_id_type=MESH).wait_recv()

            lax.fori_loop(0, 3 * SIDE, arrived, None)
            for h in range(2):
                vt_s[h, :HEAD, :] = recv[3 * w + 2, :, h * HEAD : (h + 1) * HEAD].T
                vt_s[h, HEAD:, :] = jnp.ones((16, tokens), jnp.bfloat16)
            for i in range(tokens // strip):

                def head(h, _):
                    lanes = pl.ds(pl.multiple_of(h * HEAD, HEAD), HEAD)
                    q = recv[3 * w, i * strip : (i + 1) * strip, lanes]
                    scores = [_dot(recv[3 * w + 1, b * strip : (b + 1) * strip, lanes], q, 1, 1) for b in range(i + 1)]
                    scores[i] = jnp.where(hidden, NEG, scores[i])
                    top = functools.reduce(jnp.maximum, [s.max(axis=0, keepdims=True) for s in scores])
                    mix = 0
                    for b, s in enumerate(scores):
                        weights = jnp.exp2((s - top) * e).astype(jnp.bfloat16)
                        mix = mix + _dot(vt_s[h, :, b * strip : (b + 1) * strip], weights, 1, 0)
                    seen = (mix[:HEAD] * (1 / mix[HEAD : HEAD + 1])).T.astype(jnp.bfloat16)
                    osend[w, i * strip : (i + 1) * strip, lanes] = seen

                lax.fori_loop(0, 2, head, None)
            orecv[w, 0, place] = osend[w, block(chip)]

            def give(n, _):
                give_copy(w, lax.div(n, SIDE), lax.rem(n, SIDE)).start()

            lax.fori_loop(0, CHIPS - 1, give, None)

        lax.fori_loop(0, waves, attend, None)

        def hand(p):
            return pltpu.make_async_remote_copy(acc.at[p, theirs], part.at[p], p_send.at[p], p_recv.at[p],
                                                device_id=partner, device_id_type=MESH)

        def chunk(n, _):
            w, far, p = lax.div(n, 2 * parts), lax.rem(lax.div(n, parts), 2), lax.rem(n, parts)
            slot = lax.rem(n, 3)

            @pl.when(n + 2 < chunks)
            def _():
                fetch(n + 2)

            @pl.when(p == 0)
            def _():
                def arrived(m, _):
                    c = chip_of(lax.rem(side + far, 2), m)

                    @pl.when(c != chip)
                    def _():
                        pltpu.make_async_remote_copy(osend.at[w, block(c)], orecv.at[w, far, m], o_send.at[w, 0, 0],
                                                     o_recv.at[w, far, m], device_id=at(c), device_id_type=MESH).wait_recv()

                lax.fori_loop(0, SIDE, arrived, None)

            pltpu.make_async_copy(wo.at[pl.ds(0, SIDE * TILE), pl.ds(0, wide)], slots.at[slot], slot_sem.at[slot]).wait()
            seen = jnp.concatenate([orecv[w, far, m] for m in range(SIDE)], axis=1)
            more = _dot(seen, slots[slot], 1, 0)

            @pl.when(n < parts)
            def _():
                acc[p] = more

            @pl.when(n >= parts)
            def _():
                acc[p] += more

            @pl.when(n > chunks - parts)
            def _():
                hand(p - 1).start()

        lax.fori_loop(0, chunks, chunk, None)

        def sent(r, _):
            cross_copy(r).wait_send()

        def lent_out(n, _):
            for copy in own_copies(n):
                copy.wait_send()

        lax.fori_loop(0, phase, sent, None)
        lax.fori_loop(0, groups * (SIDE - 1), lent_out, None)
        hand(parts - 1).start()

        def given(n, _):
            w, r = lax.div(n, CHIPS - 1), lax.rem(n, CHIPS - 1)
            give_copy(w, lax.div(r, SIDE), lax.rem(r, SIDE)).wait_send()

        lax.fori_loop(0, waves * (CHIPS - 1), given, None)

        def add(p, _):
            across = pl.ds(pl.multiple_of(p * wide, wide), wide)
            hand(p).wait_recv()
            total = acc[p, mine, :] + part[p]
            y_ref[:, across] = (x_v[:, across].astype(jnp.float32) + total).astype(jnp.bfloat16)
            hand(p).wait_send()

        lax.fori_loop(0, parts, add, None)

    pieces = part.shape[0]
    pl.run_scoped(finish, pltpu.VMEM((3, SIDE * TILE, d // pieces), jnp.bfloat16), pltpu.VMEM((pieces, rows, d // pieces), jnp.float32),
                  pltpu.SemaphoreType.DMA((3,)))


def _turns(tokens):
    half = HEAD // 2
    angle = np.arange(tokens, dtype=np.float32)[:, None] * np.float32(THETA) ** (-np.arange(half, dtype=np.float32) / np.float32(half))
    angle = angle.astype(np.float32).astype(np.float64)
    return np.concatenate([np.cos(angle), np.sin(angle)], 1).astype(np.float32)


def solution(mesh):
    def step(x, gain, wq, wk, wv, wo):
        own, d = x.shape
        rows, tokens = 2 * own, 2 * own * CHIPS
        waves = wq.shape[1] // (2 * CHIPS * TILE)
        groups, pieces = 3 * waves, 4
        hbm, vmem = pl.BlockSpec(memory_space=pl.ANY), pl.BlockSpec(memory_space=pltpu.VMEM)
        dma, low, f32 = pltpu.SemaphoreType.DMA, jnp.bfloat16, jnp.float32
        return pl.pallas_call(
            _kernel,
            out_shape=jax.ShapeDtypeStruct((own, d), low),
            in_specs=[hbm, vmem, hbm, hbm, hbm, hbm, hbm],
            out_specs=vmem,
            scratch_shapes=[
                pltpu.VMEM((rows + own, d), low),
                pltpu.VMEM((own, d), low),
                pltpu.VMEM((rows + own, HEAD), f32),
                pltpu.VMEM((rows + own, HEAD), f32),
                pltpu.VMEM((rows + own, HEAD), f32),
                pltpu.VMEM((groups * SIDE, own, TILE), low),
                pltpu.VMEM((groups * (SIDE - 1), rows + own, TILE), low),
                pltpu.VMEM((groups, tokens, TILE), low),
                pltpu.VMEM((waves, tokens, TILE), low),
                pltpu.VMEM((waves, 2, SIDE, rows, TILE), low),
                pltpu.VMEM((pieces, own, d // pieces), f32),
                pltpu.VMEM((2, HEAD + 16, tokens), low),
                dma((3,)),
                dma,
                dma,
                dma,
                dma,
                dma,
                dma,
                dma((groups * SIDE,)),
                dma((groups * (SIDE - 1), 2)),
                dma((groups, SIDE, 3)),
                dma((waves, 2, SIDE)),
                dma((waves, 2, SIDE)),
                dma((pieces,)),
                dma((pieces,)),
            ],
            compiler_params=pltpu.CompilerParams(collective_id=0, has_side_effects=True, vmem_limit_bytes=67043328),
        )(x, gain.reshape(1, d), _turns(tokens), wq, wk, wv, wo)

    rows, whole = P(("dp", "sp"), None), P(None, None)
    return jax.shard_map(
        step,
        mesh=mesh,
        in_specs=(rows, P(None), whole, whole, whole, whole),
        out_specs=rows,
        check_vma=False,
    )
```

```python
import functools

import jax
import jax.numpy as jnp
import numpy as np
from jax import lax
from jax.experimental import pallas as pl
from jax.experimental.pallas import tpu as pltpu
from jax.sharding import PartitionSpec as P

HEAD = 128
THETA = 10000
LOG2E = 1.4426950408889634
NEG = -1e30
MESH = pl.DeviceIdType.MESH
TILE = 256
CHIPS, SIDE = 8, 4
LATER = 9


def _dot(a, b, ca, cb):
    return lax.dot_general(a, b, (((ca,), (cb,)), ((), ())), preferred_element_type=jnp.float32)


def _kernel(x_ref, gain_ref, turn_ref, wq, wk, wv, wo, y_ref, a_v, x_v, loan_v, turn_v, cos_v, sin_v, send, lend, recv, osend, orecv, part, vt_s,
            load_sem, pair_send, pair_recv, lent_send, lent_recv, pass_send, pass_recv, c_send, l_send, q_recv, o_send, o_recv,
            p_send, p_recv):
    own, d = x_ref.shape
    rows = 2 * own
    tokens = CHIPS * rows
    waves = recv.shape[0] // 3
    groups = 3 * waves
    phase = groups * SIDE
    half = waves * CHIPS * TILE
    me = lax.axis_index("sp")
    core, chip = lax.rem(me, 2), lax.div(me, 2)
    side = lax.rem(lax.div(chip, 2), 2)
    place = lax.div(chip, SIDE) * 2 + lax.rem(chip, 2)
    other = 1 - core
    partner = {"sp": 2 * chip + other}
    at = lambda c: {"sp": 2 * c + core}
    chip_of = lambda s, m: lax.div(m, 2) * SIDE + s * 2 + lax.rem(m, 2)
    near = lambda o: lax.rem(place + 1 + o, SIDE)
    counter = chip_of(1 - side, place)
    block = lambda c: pl.ds(pl.multiple_of(rows * c, rows), rows)
    first = lambda c: pl.ds(pl.multiple_of(rows * c, own), own)
    second = lambda c: pl.ds(pl.multiple_of(rows * c + own, own), own)
    bit = own // 2
    part_of = lambda k, h: pl.ds(pl.multiple_of(own * h + bit * k, bit), bit)
    borrowed = lambda k: part_of(k, 2)

    load_x = pltpu.make_async_copy(x_ref, x_v, load_sem.at[0])
    load_turns = []
    for h in range(3):
        for k in range(2):
            row = rows * (counter if h == 2 else chip) + own * k + bit * (h % 2)
            load_turns.append(pltpu.make_async_copy(turn_ref.at[pl.ds(pl.multiple_of(row, bit), bit)], turn_v.at[part_of(k, h)],
                                                    load_sem.at[1 + 2 * h + k]))
    load_x.start()
    for copy in load_turns:
        copy.start()

    barrier = pltpu.get_barrier_semaphore()
    pl.semaphore_signal(barrier, inc=1, device_id=partner, device_id_type=MESH)

    def greet(o, _):
        pl.semaphore_signal(barrier, inc=1, device_id=at(lax.rem(chip + 1 + o, CHIPS)), device_id_type=MESH)

    lax.fori_loop(0, CHIPS - 1, greet, None)

    def cross_copy(r):
        g, o = lax.div(r, SIDE), lax.rem(r, SIDE)
        return pltpu.make_async_remote_copy(send.at[r], recv.at[g, second(chip)], c_send.at[r], q_recv.at[g, place, 2],
                                            device_id=at(chip_of(1 - side, near(o))), device_id_type=MESH)

    def own_copies(n):
        g, o = lax.div(n, SIDE - 1), lax.rem(n, SIDE - 1)
        to = at(chip_of(side, near(o)))
        return (
            pltpu.make_async_remote_copy(lend.at[n, pl.ds(0, rows)], recv.at[g, block(chip)], l_send.at[n, 0], q_recv.at[g, place, 0],
                                         device_id=to, device_id_type=MESH),
            pltpu.make_async_remote_copy(lend.at[n, pl.ds(rows, own)], recv.at[g, first(counter)], l_send.at[n, 1],
                                         q_recv.at[g, place, 1], device_id=to, device_id_type=MESH),
        )

    def project(slots, slot_sem):
        def fetch(i):
            s, r = lax.div(i, phase), lax.rem(i, phase)
            g, o = lax.div(r, SIDE), lax.rem(r, SIDE)
            w, t = lax.div(g, 3), lax.rem(g, 3)
            to = chip_of(lax.rem(side + 1 + s, 2), near(o))
            column = pl.multiple_of(half * core + (w * CHIPS + to) * TILE, TILE)
            slot = lax.rem(i, 3)
            for n, ref in enumerate((wq, wk, wv)):

                @pl.when(t == n)
                def _():
                    pltpu.make_async_copy(ref.at[:, pl.ds(column, TILE)], slots.at[slot], slot_sem.at[slot]).start()

        fetch(jnp.int32(0))
        fetch(jnp.int32(1))
        pl.semaphore_wait(barrier, CHIPS)
        lending = pltpu.make_async_remote_copy(x_ref.at[pl.ds(0, bit)], loan_v, lent_send, lent_recv, device_id=at(counter), device_id_type=MESH)
        lending.start()
        load_x.wait()

        def norm(read, base, n):
            wide = read(pl.ds(pl.multiple_of(n * 16, 16), 16)).astype(jnp.float32)
            scale = lax.rsqrt(jnp.mean(wide * wide, -1, keepdims=True) + 1e-6)
            a_v[pl.ds(pl.multiple_of(base + n * 16, 16), 16), :] = (wide * scale * gain_ref[...].astype(jnp.float32)).astype(jnp.bfloat16)

        def norm_own(n, _):
            h = lax.div(n * 16, bit)
            norm(lambda span: x_v[span, :], bit * core + (own - bit) * h, n)

        lax.fori_loop(0, own // 16, norm_own, None)
        for copy in load_turns:
            copy.wait()
        low = lax.broadcasted_iota(jnp.int32, (rows + own, HEAD), 1) < HEAD // 2
        here = turn_v[...]
        there = pltpu.roll(here, HEAD // 2, 1)
        cos_v[...] = jnp.where(low, here, there)
        sin_v[...] = jnp.where(low, -there, here)
        shares = [pltpu.make_async_remote_copy(a_v.at[part_of(core, h)], a_v.at[part_of(core, h)], pair_send.at[h], pair_recv.at[h],
                                               device_id=partner, device_id_type=MESH) for h in range(2)]
        for copy in shares:
            copy.start()
        for copy in shares:
            copy.wait()

        def tile(i, high, low, store):
            slot = lax.rem(i, 3)
            t = lax.rem(lax.div(i, SIDE), 3)
            pltpu.make_async_copy(wq.at[:, pl.ds(0, TILE)], slots.at[slot], slot_sem.at[slot]).wait()

            @pl.when(i + 2 < 2 * phase)
            def _():
                fetch(i + 2)

            got = _dot(a_v[low:high, :], slots[slot], 1, 0).astype(jnp.bfloat16)
            for h in range(TILE // HEAD):
                cols = slice(h * HEAD, (h + 1) * HEAD)

                @pl.when(t < 2)
                def _():
                    wide = got[:, cols].astype(jnp.float32)
                    turned = wide * cos_v[low:high, :] + pltpu.roll(wide, HEAD // 2, 1) * sin_v[low:high, :]
                    store(turned.astype(jnp.bfloat16), cols)

                @pl.when(t == 2)
                def _():
                    store(got[:, cols], cols)

        def cross(r, _):
            def store(value, cols):
                send[r, :, cols] = value

            tile(r, rows, own, store)

        lax.fori_loop(0, phase, cross, None)
        lending.wait_recv()

        def send_cross(r, _):
            cross_copy(r).start()

        lax.fori_loop(0, phase // 2, send_cross, None)

        def norm_loan(n, _):
            norm(lambda span: loan_v[span, :], rows + bit * core, n)

        lax.fori_loop(0, bit // 16, norm_loan, None)
        passing = pltpu.make_async_remote_copy(a_v.at[borrowed(core)], a_v.at[borrowed(core)], pass_send, pass_recv,
                                               device_id=partner, device_id_type=MESH)
        passing.start()
        passing.wait()
        lending.wait_send()

        def within(r, _):
            g, o = lax.div(r, SIDE), lax.rem(r, SIDE)
            n = g * (SIDE - 1) + o

            def store(value, cols):
                @pl.when(o < SIDE - 1)
                def _():
                    lend[n, :, cols] = value

                @pl.when(o == SIDE - 1)
                def _():
                    recv[g, block(chip), cols] = value[:rows]
                    recv[g, first(counter), cols] = value[rows:]

            tile(phase + r, rows + own, 0, store)

            @pl.when((r >= LATER) & (r < LATER + phase // 2))
            def _():
                cross_copy(phase // 2 + r - LATER).start()

            @pl.when(o > 0)
            def _():
                for copy in own_copies(n - 1):
                    copy.start()

        lax.fori_loop(0, phase, within, None)

    pl.run_scoped(project, pltpu.VMEM((3, d, TILE), jnp.bfloat16), pltpu.SemaphoreType.DMA((3,)))

    def give_copy(w, s, o):
        c = chip_of(lax.rem(side + 1 + s, 2), near(o))
        return pltpu.make_async_remote_copy(osend.at[w, block(c)], orecv.at[w, lax.rem(1 + s, 2), place], o_send.at[w, s, o],
                                            o_recv.at[w, lax.rem(1 + s, 2), place], device_id=at(c), device_id_type=MESH)

    def finish(slots, acc, slot_sem):
        parts, wide = acc.shape[0], acc.shape[2]
        chunks = waves * 2 * parts

        def fetch(n):
            w, far, p = lax.div(n, 2 * parts), lax.rem(lax.div(n, parts), 2), lax.rem(n, parts)
            slot = lax.rem(n, 3)
            across = pl.ds(pl.multiple_of(p * wide, wide), wide)

            def source(m, _):
                row = pl.multiple_of(half * core + (w * CHIPS + chip_of(lax.rem(side + far, 2), m)) * TILE, TILE)
                into = pl.ds(pl.multiple_of(m * TILE, TILE), TILE)
                pltpu.make_async_copy(wo.at[pl.ds(row, TILE), across], slots.at[slot, into], slot_sem.at[slot]).start()

            lax.fori_loop(0, SIDE, source, None)

        fetch(jnp.int32(0))
        fetch(jnp.int32(1))

        strip = 512

        def position(axis):
            r = lax.broadcasted_iota(jnp.int32, (strip, strip), axis)
            c, h, k = lax.div(r, rows), lax.rem(lax.div(r, own), 2), lax.rem(lax.div(r, bit), 2)
            return c * rows + k * own + h * bit + lax.rem(r, bit)

        hidden = position(0) > position(1)
        e = HEAD**-0.5 * LOG2E

        def attend(w, _):
            def arrived(n, _):
                g, o = 3 * w + lax.div(n, SIDE), lax.rem(n, SIDE)
                m = near(o)

                @pl.when(o < SIDE - 1)
                def _():
                    c = chip_of(side, m)
                    pltpu.make_async_remote_copy(lend.at[0, pl.ds(0, rows)], recv.at[g, block(c)], l_send.at[0, 0], q_recv.at[g, m, 0],
                                                 device_id=at(c), device_id_type=MESH).wait_recv()
                    pltpu.make_async_remote_copy(lend.at[0, pl.ds(rows, own)], recv.at[g, first(chip_of(1 - side, m))], l_send.at[0, 1],
                                                 q_recv.at[g, m, 1], device_id=at(c), device_id_type=MESH).wait_recv()

                c = chip_of(1 - side, m)
                pltpu.make_async_remote_copy(send.at[0], recv.at[g, second(c)], c_send.at[0], q_recv.at[g, m, 2],
                                             device_id=at(c), device_id_type=MESH).wait_recv()

            lax.fori_loop(0, 3 * SIDE, arrived, None)
            for h in range(2):
                vt_s[h, :HEAD, :] = recv[3 * w + 2, :, h * HEAD : (h + 1) * HEAD].T
                vt_s[h, HEAD:, :] = jnp.ones((16, tokens), jnp.bfloat16)
            for i in range(tokens // strip):

                def head(h, _):
                    lanes = pl.ds(pl.multiple_of(h * HEAD, HEAD), HEAD)
                    q = recv[3 * w, i * strip : (i + 1) * strip, lanes]
                    scores = [_dot(recv[3 * w + 1, b * strip : (b + 1) * strip, lanes], q, 1, 1) for b in range(i + 1)]
                    scores[i] = jnp.where(hidden, NEG, scores[i])
                    top = functools.reduce(jnp.maximum, [s.max(axis=0, keepdims=True) for s in scores])
                    mix = 0
                    for b, s in enumerate(scores):
                        weights = jnp.exp2((s - top) * e).astype(jnp.bfloat16)
                        mix = mix + _dot(vt_s[h, :, b * strip : (b + 1) * strip], weights, 1, 0)
                    seen = (mix[:HEAD] * (1 / mix[HEAD : HEAD + 1])).T.astype(jnp.bfloat16)
                    osend[w, i * strip : (i + 1) * strip, lanes] = seen

                lax.fori_loop(0, 2, head, None)
            orecv[w, 0, place] = osend[w, block(chip)]

            def give(n, _):
                give_copy(w, lax.div(n, SIDE), lax.rem(n, SIDE)).start()

            lax.fori_loop(0, CHIPS - 1, give, None)

        lax.fori_loop(0, waves, attend, None)

        def hand(p):
            return [pltpu.make_async_remote_copy(acc.at[p, part_of(other, h)], part.at[p, pl.ds(bit * h, bit)], p_send.at[p, h],
                                                 p_recv.at[p, h], device_id=partner, device_id_type=MESH) for h in range(2)]

        def chunk(n, _):
            w, far, p = lax.div(n, 2 * parts), lax.rem(lax.div(n, parts), 2), lax.rem(n, parts)
            slot = lax.rem(n, 3)

            @pl.when(n + 2 < chunks)
            def _():
                fetch(n + 2)

            @pl.when(p == 0)
            def _():
                def arrived(m, _):
                    c = chip_of(lax.rem(side + far, 2), m)

                    @pl.when(c != chip)
                    def _():
                        pltpu.make_async_remote_copy(osend.at[w, block(c)], orecv.at[w, far, m], o_send.at[w, 0, 0],
                                                     o_recv.at[w, far, m], device_id=at(c), device_id_type=MESH).wait_recv()

                lax.fori_loop(0, SIDE, arrived, None)

            pltpu.make_async_copy(wo.at[pl.ds(0, SIDE * TILE), pl.ds(0, wide)], slots.at[slot], slot_sem.at[slot]).wait()
            seen = jnp.concatenate([orecv[w, far, m] for m in range(SIDE)], axis=1)
            more = _dot(seen, slots[slot], 1, 0)

            @pl.when(n < parts)
            def _():
                acc[p] = more

            @pl.when(n >= parts)
            def _():
                acc[p] += more

            @pl.when(n > chunks - parts)
            def _():
                for copy in hand(p - 1):
                    copy.start()

        lax.fori_loop(0, chunks, chunk, None)

        def sent(r, _):
            cross_copy(r).wait_send()

        def lent_out(n, _):
            for copy in own_copies(n):
                copy.wait_send()

        lax.fori_loop(0, phase, sent, None)
        lax.fori_loop(0, groups * (SIDE - 1), lent_out, None)
        for copy in hand(parts - 1):
            copy.start()

        def given(n, _):
            w, r = lax.div(n, CHIPS - 1), lax.rem(n, CHIPS - 1)
            give_copy(w, lax.div(r, SIDE), lax.rem(r, SIDE)).wait_send()

        lax.fori_loop(0, waves * (CHIPS - 1), given, None)

        def add(p, _):
            across = pl.ds(pl.multiple_of(p * wide, wide), wide)
            for h, copy in enumerate(hand(p)):
                copy.wait_recv()
                span = slice(bit * h, bit * (h + 1))
                total = acc[p, part_of(core, h), :] + part[p, span]
                y_ref[span, across] = (x_v[span, across].astype(jnp.float32) + total).astype(jnp.bfloat16)
                copy.wait_send()

        lax.fori_loop(0, parts, add, None)

    pieces = part.shape[0]
    pl.run_scoped(finish, pltpu.VMEM((3, SIDE * TILE, d // pieces), jnp.bfloat16), pltpu.VMEM((pieces, rows, d // pieces), jnp.float32),
                  pltpu.SemaphoreType.DMA((3,)))


def _turns(tokens):
    half = HEAD // 2
    angle = np.arange(tokens, dtype=np.float32)[:, None] * np.float32(THETA) ** (-np.arange(half, dtype=np.float32) / np.float32(half))
    angle = angle.astype(np.float32).astype(np.float64)
    return np.concatenate([np.cos(angle), np.sin(angle)], 1).astype(np.float32)


def solution(mesh):
    def step(x, gain, wq, wk, wv, wo):
        own, d = x.shape
        rows, tokens = 2 * own, 2 * own * CHIPS
        waves = wq.shape[1] // (2 * CHIPS * TILE)
        groups, pieces = 3 * waves, 4
        hbm, vmem = pl.BlockSpec(memory_space=pl.ANY), pl.BlockSpec(memory_space=pltpu.VMEM)
        dma, low, f32 = pltpu.SemaphoreType.DMA, jnp.bfloat16, jnp.float32
        return pl.pallas_call(
            _kernel,
            out_shape=jax.ShapeDtypeStruct((own, d), low),
            in_specs=[hbm, vmem, hbm, hbm, hbm, hbm, hbm],
            out_specs=vmem,
            scratch_shapes=[
                pltpu.VMEM((rows + own, d), low),
                pltpu.VMEM((own, d), low),
                pltpu.VMEM((own // 2, d), low),
                pltpu.VMEM((rows + own, HEAD), f32),
                pltpu.VMEM((rows + own, HEAD), f32),
                pltpu.VMEM((rows + own, HEAD), f32),
                pltpu.VMEM((groups * SIDE, own, TILE), low),
                pltpu.VMEM((groups * (SIDE - 1), rows + own, TILE), low),
                pltpu.VMEM((groups, tokens, TILE), low),
                pltpu.VMEM((waves, tokens, TILE), low),
                pltpu.VMEM((waves, 2, SIDE, rows, TILE), low),
                pltpu.VMEM((pieces, own, d // pieces), f32),
                pltpu.VMEM((2, HEAD + 16, tokens), low),
                dma((7,)),
                dma((2,)),
                dma((2,)),
                dma,
                dma,
                dma,
                dma,
                dma((groups * SIDE,)),
                dma((groups * (SIDE - 1), 2)),
                dma((groups, SIDE, 3)),
                dma((waves, 2, SIDE)),
                dma((waves, 2, SIDE)),
                dma((pieces, 2)),
                dma((pieces, 2)),
            ],
            compiler_params=pltpu.CompilerParams(collective_id=0, has_side_effects=True, vmem_limit_bytes=67043328),
        )(x, gain.reshape(1, d), _turns(tokens), wq, wk, wv, wo)

    rows, whole = P(("dp", "sp"), None), P(None, None)
    return jax.shard_map(
        step,
        mesh=mesh,
        in_specs=(rows, P(None), whole, whole, whole, whole),
        out_specs=rows,
        check_vma=False,
    )
```

```python
import functools

import jax
import jax.numpy as jnp
import numpy as np
from jax import lax
from jax.experimental import pallas as pl
from jax.experimental.pallas import tpu as pltpu
from jax.sharding import PartitionSpec as P

HEAD = 128
THETA = 10000
LOG2E = 1.4426950408889634
NEG = -1e30
MESH = pl.DeviceIdType.MESH
TILE = 256
CHIPS, SIDE = 8, 4
LATER = 9


def _dot(a, b, ca, cb):
    return lax.dot_general(a, b, (((ca,), (cb,)), ((), ())), preferred_element_type=jnp.float32)


def _kernel(x_ref, gain_ref, turn_ref, wq, wk, wv, wo, y_ref, a_v, x_v, gain_v, loan_v, turn_v, cos_v, sin_v, send, lend, recv, osend, orecv, part, vt_s,
            load_sem, pair_send, pair_recv, lent_send, lent_recv, pass_send, pass_recv, c_send, l_send, q_recv, o_send, o_recv,
            p_send, p_recv):
    own, d = x_ref.shape
    rows = 2 * own
    tokens = CHIPS * rows
    waves = recv.shape[0] // 3
    groups = 3 * waves
    phase = groups * SIDE
    half = waves * CHIPS * TILE
    me = lax.axis_index("sp")
    core, chip = lax.rem(me, 2), lax.div(me, 2)
    side = lax.rem(lax.div(chip, 2), 2)
    place = lax.div(chip, SIDE) * 2 + lax.rem(chip, 2)
    other = 1 - core
    partner = {"sp": 2 * chip + other}
    at = lambda c: {"sp": 2 * c + core}
    chip_of = lambda s, m: lax.div(m, 2) * SIDE + s * 2 + lax.rem(m, 2)
    near = lambda o: lax.rem(place + 1 + o, SIDE)
    counter = chip_of(1 - side, place)
    block = lambda c: pl.ds(pl.multiple_of(rows * c, rows), rows)
    first = lambda c: pl.ds(pl.multiple_of(rows * c, own), own)
    second = lambda c: pl.ds(pl.multiple_of(rows * c + own, own), own)
    bit = own // 2
    part_of = lambda k, h: pl.ds(pl.multiple_of(own * h + bit * k, bit), bit)
    borrowed = lambda k: part_of(k, 2)

    load_x = pltpu.make_async_copy(x_ref, x_v, load_sem.at[0])
    load_turns = []
    for h in range(3):
        for k in range(2):
            row = rows * (counter if h == 2 else chip) + own * k + bit * (h % 2)
            load_turns.append(pltpu.make_async_copy(turn_ref.at[pl.ds(pl.multiple_of(row, bit), bit)], turn_v.at[part_of(k, h)],
                                                    load_sem.at[1 + 2 * h + k]))
    load_x.start()
    for copy in load_turns:
        copy.start()

    barrier = pltpu.get_barrier_semaphore()
    pl.semaphore_signal(barrier, inc=1, device_id=partner, device_id_type=MESH)

    def greet(o, _):
        pl.semaphore_signal(barrier, inc=1, device_id=at(lax.rem(chip + 1 + o, CHIPS)), device_id_type=MESH)

    lax.fori_loop(0, CHIPS - 1, greet, None)

    def cross_copy(r):
        g, o = lax.div(r, SIDE), lax.rem(r, SIDE)
        return pltpu.make_async_remote_copy(send.at[r], recv.at[g, second(chip)], c_send.at[r], q_recv.at[g, place, 2],
                                            device_id=at(chip_of(1 - side, near(o))), device_id_type=MESH)

    def own_copies(n):
        g, o = lax.div(n, SIDE - 1), lax.rem(n, SIDE - 1)
        to = at(chip_of(side, near(o)))
        return (
            pltpu.make_async_remote_copy(lend.at[n, pl.ds(0, rows)], recv.at[g, block(chip)], l_send.at[n, 0], q_recv.at[g, place, 0],
                                         device_id=to, device_id_type=MESH),
            pltpu.make_async_remote_copy(lend.at[n, pl.ds(rows, own)], recv.at[g, first(counter)], l_send.at[n, 1],
                                         q_recv.at[g, place, 1], device_id=to, device_id_type=MESH),
        )

    def project(slots, slot_sem):
        def fetch(i):
            s, r = lax.div(i, phase), lax.rem(i, phase)
            g, o = lax.div(r, SIDE), lax.rem(r, SIDE)
            w, t = lax.div(g, 3), lax.rem(g, 3)
            to = chip_of(lax.rem(side + 1 + s, 2), near(o))
            column = pl.multiple_of(half * core + (w * CHIPS + to) * TILE, TILE)
            slot = lax.rem(i, 3)
            for n, ref in enumerate((wq, wk, wv)):

                @pl.when(t == n)
                def _():
                    pltpu.make_async_copy(ref.at[:, pl.ds(column, TILE)], slots.at[slot], slot_sem.at[slot]).start()

        fetch(jnp.int32(0))
        fetch(jnp.int32(1))
        pl.semaphore_wait(barrier, CHIPS)
        lending = pltpu.make_async_remote_copy(x_ref.at[pl.ds(0, bit)], loan_v, lent_send, lent_recv, device_id=at(counter), device_id_type=MESH)
        lending.start()
        gain_v[...] = gain_ref[...].reshape(1, d).astype(jnp.float32)
        load_x.wait()

        def norm(read, base, n):
            wide = read(pl.ds(pl.multiple_of(n * 16, 16), 16)).astype(jnp.float32)
            scale = lax.rsqrt(jnp.mean(wide * wide, -1, keepdims=True) + 1e-6)
            a_v[pl.ds(pl.multiple_of(base + n * 16, 16), 16), :] = (wide * scale * gain_v[...]).astype(jnp.bfloat16)

        def norm_own(n, _):
            h = lax.div(n * 16, bit)
            norm(lambda span: x_v[span, :], bit * core + (own - bit) * h, n)

        lax.fori_loop(0, own // 16, norm_own, None)
        for copy in load_turns:
            copy.wait()
        low = lax.broadcasted_iota(jnp.int32, (rows + own, HEAD), 1) < HEAD // 2
        here = turn_v[...]
        there = pltpu.roll(here, HEAD // 2, 1)
        cos_v[...] = jnp.where(low, here, there)
        sin_v[...] = jnp.where(low, -there, here)
        shares = [pltpu.make_async_remote_copy(a_v.at[part_of(core, h)], a_v.at[part_of(core, h)], pair_send.at[h], pair_recv.at[h],
                                               device_id=partner, device_id_type=MESH) for h in range(2)]
        for copy in shares:
            copy.start()
        for copy in shares:
            copy.wait()

        def tile(i, high, low, store):
            slot = lax.rem(i, 3)
            t = lax.rem(lax.div(i, SIDE), 3)
            pltpu.make_async_copy(wq.at[:, pl.ds(0, TILE)], slots.at[slot], slot_sem.at[slot]).wait()

            @pl.when(i + 2 < 2 * phase)
            def _():
                fetch(i + 2)

            got = _dot(a_v[low:high, :], slots[slot], 1, 0).astype(jnp.bfloat16)
            for h in range(TILE // HEAD):
                cols = slice(h * HEAD, (h + 1) * HEAD)

                @pl.when(t < 2)
                def _():
                    wide = got[:, cols].astype(jnp.float32)
                    turned = wide * cos_v[low:high, :] + pltpu.roll(wide, HEAD // 2, 1) * sin_v[low:high, :]
                    store(turned.astype(jnp.bfloat16), cols)

                @pl.when(t == 2)
                def _():
                    store(got[:, cols], cols)

        def cross(r, _):
            def store(value, cols):
                send[r, :, cols] = value

            tile(r, rows, own, store)

        lax.fori_loop(0, phase, cross, None)
        lending.wait_recv()

        def send_cross(r, _):
            cross_copy(r).start()

        lax.fori_loop(0, phase // 2, send_cross, None)

        def norm_loan(n, _):
            norm(lambda span: loan_v[span, :], rows + bit * core, n)

        lax.fori_loop(0, bit // 16, norm_loan, None)
        passing = pltpu.make_async_remote_copy(a_v.at[borrowed(core)], a_v.at[borrowed(core)], pass_send, pass_recv,
                                               device_id=partner, device_id_type=MESH)
        passing.start()
        passing.wait()
        lending.wait_send()

        def within(r, _):
            g, o = lax.div(r, SIDE), lax.rem(r, SIDE)
            n = g * (SIDE - 1) + o

            def store(value, cols):
                @pl.when(o < SIDE - 1)
                def _():
                    lend[n, :, cols] = value

                @pl.when(o == SIDE - 1)
                def _():
                    recv[g, block(chip), cols] = value[:rows]
                    recv[g, first(counter), cols] = value[rows:]

            tile(phase + r, rows + own, 0, store)

            @pl.when((r >= LATER) & (r < LATER + phase // 2))
            def _():
                cross_copy(phase // 2 + r - LATER).start()

            @pl.when(o > 0)
            def _():
                for copy in own_copies(n - 1):
                    copy.start()

        lax.fori_loop(0, phase, within, None)

    pl.run_scoped(project, pltpu.VMEM((3, d, TILE), jnp.bfloat16), pltpu.SemaphoreType.DMA((3,)))

    def give_copy(w, s, o):
        c = chip_of(lax.rem(side + 1 + s, 2), near(o))
        return pltpu.make_async_remote_copy(osend.at[w, block(c)], orecv.at[w, lax.rem(1 + s, 2), place], o_send.at[w, s, o],
                                            o_recv.at[w, lax.rem(1 + s, 2), place], device_id=at(c), device_id_type=MESH)

    def finish(slots, acc, slot_sem):
        parts, wide = acc.shape[0], acc.shape[2]
        chunks = waves * 2 * parts

        def fetch(n):
            w, far, p = lax.div(n, 2 * parts), lax.rem(lax.div(n, parts), 2), lax.rem(n, parts)
            slot = lax.rem(n, 3)
            across = pl.ds(pl.multiple_of(p * wide, wide), wide)

            def source(m, _):
                row = pl.multiple_of(half * core + (w * CHIPS + chip_of(lax.rem(side + far, 2), m)) * TILE, TILE)
                into = pl.ds(pl.multiple_of(m * TILE, TILE), TILE)
                pltpu.make_async_copy(wo.at[pl.ds(row, TILE), across], slots.at[slot, into], slot_sem.at[slot]).start()

            lax.fori_loop(0, SIDE, source, None)

        fetch(jnp.int32(0))
        fetch(jnp.int32(1))

        strip = 512

        def position(axis):
            r = lax.broadcasted_iota(jnp.int32, (strip, strip), axis)
            c, h, k = lax.div(r, rows), lax.rem(lax.div(r, own), 2), lax.rem(lax.div(r, bit), 2)
            return c * rows + k * own + h * bit + lax.rem(r, bit)

        hidden = position(0) > position(1)
        e = HEAD**-0.5 * LOG2E

        def give(w):
            def one(n, _):
                give_copy(w, lax.div(n, SIDE), lax.rem(n, SIDE)).start()

            lax.fori_loop(0, CHIPS - 1, one, None)

        def attend(w, _):
            def arrived(n, _):
                g, o = 3 * w + lax.div(n, SIDE), lax.rem(n, SIDE)
                m = near(o)

                @pl.when(o < SIDE - 1)
                def _():
                    c = chip_of(side, m)
                    pltpu.make_async_remote_copy(lend.at[0, pl.ds(0, rows)], recv.at[g, block(c)], l_send.at[0, 0], q_recv.at[g, m, 0],
                                                 device_id=at(c), device_id_type=MESH).wait_recv()
                    pltpu.make_async_remote_copy(lend.at[0, pl.ds(rows, own)], recv.at[g, first(chip_of(1 - side, m))], l_send.at[0, 1],
                                                 q_recv.at[g, m, 1], device_id=at(c), device_id_type=MESH).wait_recv()

                c = chip_of(1 - side, m)
                pltpu.make_async_remote_copy(send.at[0], recv.at[g, second(c)], c_send.at[0], q_recv.at[g, m, 2],
                                             device_id=at(c), device_id_type=MESH).wait_recv()

            lax.fori_loop(0, 3 * SIDE, arrived, None)

            @pl.when(w > 0)
            def _():
                give(w - 1)

            for h in range(2):
                vt_s[h, :HEAD, :] = recv[3 * w + 2, :, h * HEAD : (h + 1) * HEAD].T
                vt_s[h, HEAD:, :] = jnp.ones((16, tokens), jnp.bfloat16)
            for i in range(tokens // strip):

                def head(h, _):
                    lanes = pl.ds(pl.multiple_of(h * HEAD, HEAD), HEAD)
                    q = recv[3 * w, i * strip : (i + 1) * strip, lanes]
                    scores = [_dot(recv[3 * w + 1, b * strip : (b + 1) * strip, lanes], q, 1, 1) for b in range(i + 1)]
                    scores[i] = jnp.where(hidden, NEG, scores[i])
                    top = functools.reduce(jnp.maximum, [s.max(axis=0, keepdims=True) for s in scores])
                    mix = 0
                    for b, s in enumerate(scores):
                        weights = jnp.exp2((s - top) * e).astype(jnp.bfloat16)
                        mix = mix + _dot(vt_s[h, :, b * strip : (b + 1) * strip], weights, 1, 0)
                    seen = (mix[:HEAD] * (1 / mix[HEAD : HEAD + 1])).T.astype(jnp.bfloat16)
                    osend[w, i * strip : (i + 1) * strip, lanes] = seen

                lax.fori_loop(0, 2, head, None)
            orecv[w, 0, place] = osend[w, block(chip)]

        lax.fori_loop(0, waves, attend, None)
        give(waves - 1)

        def hand(p):
            return [pltpu.make_async_remote_copy(acc.at[p, part_of(other, h)], part.at[p, pl.ds(bit * h, bit)], p_send.at[p, h],
                                                 p_recv.at[p, h], device_id=partner, device_id_type=MESH) for h in range(2)]

        def chunk(n, _):
            w, far, p = lax.div(n, 2 * parts), lax.rem(lax.div(n, parts), 2), lax.rem(n, parts)
            slot = lax.rem(n, 3)

            @pl.when(n + 2 < chunks)
            def _():
                fetch(n + 2)

            @pl.when(p == 0)
            def _():
                def arrived(m, _):
                    c = chip_of(lax.rem(side + far, 2), m)

                    @pl.when(c != chip)
                    def _():
                        pltpu.make_async_remote_copy(osend.at[w, block(c)], orecv.at[w, far, m], o_send.at[w, 0, 0],
                                                     o_recv.at[w, far, m], device_id=at(c), device_id_type=MESH).wait_recv()

                lax.fori_loop(0, SIDE, arrived, None)

            pltpu.make_async_copy(wo.at[pl.ds(0, SIDE * TILE), pl.ds(0, wide)], slots.at[slot], slot_sem.at[slot]).wait()
            seen = jnp.concatenate([orecv[w, far, m] for m in range(SIDE)], axis=1)
            more = _dot(seen, slots[slot], 1, 0)

            @pl.when(n < parts)
            def _():
                acc[p] = more

            @pl.when(n >= parts)
            def _():
                acc[p] += more

            @pl.when(n > chunks - parts)
            def _():
                for copy in hand(p - 1):
                    copy.start()

        lax.fori_loop(0, chunks, chunk, None)

        def sent(r, _):
            cross_copy(r).wait_send()

        def lent_out(n, _):
            for copy in own_copies(n):
                copy.wait_send()

        lax.fori_loop(0, phase, sent, None)
        lax.fori_loop(0, groups * (SIDE - 1), lent_out, None)
        for copy in hand(parts - 1):
            copy.start()

        def given(n, _):
            w, r = lax.div(n, CHIPS - 1), lax.rem(n, CHIPS - 1)
            give_copy(w, lax.div(r, SIDE), lax.rem(r, SIDE)).wait_send()

        lax.fori_loop(0, waves * (CHIPS - 1), given, None)

        def add(p, _):
            across = pl.ds(pl.multiple_of(p * wide, wide), wide)
            for h, copy in enumerate(hand(p)):
                copy.wait_recv()
                span = slice(bit * h, bit * (h + 1))
                total = acc[p, part_of(core, h), :] + part[p, span]
                y_ref[span, across] = (x_v[span, across].astype(jnp.float32) + total).astype(jnp.bfloat16)
                copy.wait_send()

        lax.fori_loop(0, parts, add, None)

    pieces = part.shape[0]
    pl.run_scoped(finish, pltpu.VMEM((3, SIDE * TILE, d // pieces), jnp.bfloat16), pltpu.VMEM((pieces, rows, d // pieces), jnp.float32),
                  pltpu.SemaphoreType.DMA((3,)))


def _turns(tokens):
    half = HEAD // 2
    angle = np.arange(tokens, dtype=np.float32)[:, None] * np.float32(THETA) ** (-np.arange(half, dtype=np.float32) / np.float32(half))
    angle = angle.astype(np.float32).astype(np.float64)
    return np.concatenate([np.cos(angle), np.sin(angle)], 1).astype(np.float32)


def solution(mesh):
    def step(x, gain, wq, wk, wv, wo):
        own, d = x.shape
        rows, tokens = 2 * own, 2 * own * CHIPS
        waves = wq.shape[1] // (2 * CHIPS * TILE)
        groups, pieces = 3 * waves, 4
        hbm, vmem = pl.BlockSpec(memory_space=pl.ANY), pl.BlockSpec(memory_space=pltpu.VMEM)
        dma, low, f32 = pltpu.SemaphoreType.DMA, jnp.bfloat16, jnp.float32
        return pl.pallas_call(
            _kernel,
            out_shape=jax.ShapeDtypeStruct((own, d), low),
            in_specs=[hbm, vmem, hbm, hbm, hbm, hbm, hbm],
            out_specs=vmem,
            scratch_shapes=[
                pltpu.VMEM((rows + own, d), low),
                pltpu.VMEM((own, d), low),
                pltpu.VMEM((1, d), f32),
                pltpu.VMEM((own // 2, d), low),
                pltpu.VMEM((rows + own, HEAD), f32),
                pltpu.VMEM((rows + own, HEAD), f32),
                pltpu.VMEM((rows + own, HEAD), f32),
                pltpu.VMEM((groups * SIDE, own, TILE), low),
                pltpu.VMEM((groups * (SIDE - 1), rows + own, TILE), low),
                pltpu.VMEM((groups, tokens, TILE), low),
                pltpu.VMEM((waves, tokens, TILE), low),
                pltpu.VMEM((waves, 2, SIDE, rows, TILE), low),
                pltpu.VMEM((pieces, own, d // pieces), f32),
                pltpu.VMEM((2, HEAD + 16, tokens), low),
                dma((7,)),
                dma((2,)),
                dma((2,)),
                dma,
                dma,
                dma,
                dma,
                dma((groups * SIDE,)),
                dma((groups * (SIDE - 1), 2)),
                dma((groups, SIDE, 3)),
                dma((waves, 2, SIDE)),
                dma((waves, 2, SIDE)),
                dma((pieces, 2)),
                dma((pieces, 2)),
            ],
            compiler_params=pltpu.CompilerParams(collective_id=0, has_side_effects=True, vmem_limit_bytes=67043328),
        )(x, gain, _turns(tokens), wq, wk, wv, wo)

    rows, whole = P(("dp", "sp"), None), P(None, None)
    return jax.shard_map(
        step,
        mesh=mesh,
        in_specs=(rows, P(None), whole, whole, whole, whole),
        out_specs=rows,
        check_vma=False,
    )
```

```python
import functools

import jax
import jax.numpy as jnp
import numpy as np
from jax import lax
from jax.experimental import pallas as pl
from jax.experimental.pallas import tpu as pltpu
from jax.sharding import PartitionSpec as P

HEAD = 128
THETA = 10000
LOG2E = 1.4426950408889634
NEG = -1e30
MESH = pl.DeviceIdType.MESH
TILE = 256
CHIPS, SIDE = 8, 4
LATER = 6


def _dot(a, b, ca, cb):
    return lax.dot_general(a, b, (((ca,), (cb,)), ((), ())), preferred_element_type=jnp.float32)


def _kernel(x_ref, gain_ref, turn_ref, wq, wk, wv, wo, y_ref, a_v, x_v, gain_v, loan_v, turn_v, cos_v, sin_v, send, lend, recv, osend, orecv, part, vt_s,
            load_sem, pair_send, pair_recv, lent_send, lent_recv, pass_send, pass_recv, c_send, l_send, q_recv, o_send, o_recv,
            p_send, p_recv):
    own, d = x_ref.shape
    rows = 2 * own
    tokens = CHIPS * rows
    waves = recv.shape[0] // 3
    groups = 3 * waves
    phase = groups * SIDE
    half = waves * CHIPS * TILE
    me = lax.axis_index("sp")
    core, chip = lax.rem(me, 2), lax.div(me, 2)
    side = lax.rem(lax.div(chip, 2), 2)
    place = lax.div(chip, SIDE) * 2 + lax.rem(chip, 2)
    other = 1 - core
    partner = {"sp": 2 * chip + other}
    at = lambda c: {"sp": 2 * c + core}
    chip_of = lambda s, m: lax.div(m, 2) * SIDE + s * 2 + lax.rem(m, 2)
    near = lambda o: lax.rem(place + 1 + o, SIDE)
    counter = chip_of(1 - side, place)
    block = lambda c: pl.ds(pl.multiple_of(rows * c, rows), rows)
    first = lambda c: pl.ds(pl.multiple_of(rows * c, own), own)
    second = lambda c: pl.ds(pl.multiple_of(rows * c + own, own), own)
    bit = own // 2
    part_of = lambda k, h: pl.ds(pl.multiple_of(own * h + bit * k, bit), bit)
    borrowed = lambda k: part_of(k, 2)

    load_x = pltpu.make_async_copy(x_ref, x_v, load_sem.at[0])
    load_turns = []
    for h in range(3):
        for k in range(2):
            row = rows * (counter if h == 2 else chip) + own * k + bit * (h % 2)
            load_turns.append(pltpu.make_async_copy(turn_ref.at[pl.ds(pl.multiple_of(row, bit), bit)], turn_v.at[part_of(k, h)],
                                                    load_sem.at[1 + 2 * h + k]))
    load_x.start()
    for copy in load_turns:
        copy.start()

    barrier = pltpu.get_barrier_semaphore()
    pl.semaphore_signal(barrier, inc=1, device_id=partner, device_id_type=MESH)

    def greet(o, _):
        pl.semaphore_signal(barrier, inc=1, device_id=at(lax.rem(chip + 1 + o, CHIPS)), device_id_type=MESH)

    lax.fori_loop(0, CHIPS - 1, greet, None)

    def cross_copy(r):
        g, o = lax.div(r, SIDE), lax.rem(r, SIDE)
        return pltpu.make_async_remote_copy(send.at[r], recv.at[g, second(chip)], c_send.at[r], q_recv.at[g, place, 2],
                                            device_id=at(chip_of(1 - side, near(o))), device_id_type=MESH)

    def own_copies(n):
        g, o = lax.div(n, SIDE - 1), lax.rem(n, SIDE - 1)
        to = at(chip_of(side, near(o)))
        return (
            pltpu.make_async_remote_copy(lend.at[n, pl.ds(0, rows)], recv.at[g, block(chip)], l_send.at[n, 0], q_recv.at[g, place, 0],
                                         device_id=to, device_id_type=MESH),
            pltpu.make_async_remote_copy(lend.at[n, pl.ds(rows, own)], recv.at[g, first(counter)], l_send.at[n, 1],
                                         q_recv.at[g, place, 1], device_id=to, device_id_type=MESH),
        )

    def project(slots, slot_sem):
        def fetch(i):
            s, r = lax.div(i, phase), lax.rem(i, phase)
            g, o = lax.div(r, SIDE), lax.rem(r, SIDE)
            w, t = lax.div(g, 3), lax.rem(g, 3)
            to = chip_of(lax.rem(side + s, 2), near(o))
            column = pl.multiple_of(half * core + (w * CHIPS + to) * TILE, TILE)
            slot = lax.rem(i, 3)
            for n, ref in enumerate((wq, wk, wv)):

                @pl.when(t == n)
                def _():
                    pltpu.make_async_copy(ref.at[:, pl.ds(column, TILE)], slots.at[slot], slot_sem.at[slot]).start()

        fetch(jnp.int32(0))
        fetch(jnp.int32(1))
        pl.semaphore_wait(barrier, CHIPS)
        lending = pltpu.make_async_remote_copy(x_ref.at[pl.ds(0, bit)], loan_v, lent_send, lent_recv, device_id=at(counter), device_id_type=MESH)
        lending.start()
        gain_v[...] = gain_ref[...].reshape(1, d).astype(jnp.float32)
        load_x.wait()

        def norm(read, base, n):
            wide = read(pl.ds(pl.multiple_of(n * 16, 16), 16)).astype(jnp.float32)
            scale = lax.rsqrt(jnp.mean(wide * wide, -1, keepdims=True) + 1e-6)
            a_v[pl.ds(pl.multiple_of(base + n * 16, 16), 16), :] = (wide * scale * gain_v[...]).astype(jnp.bfloat16)

        def norm_own(n, _):
            h = lax.div(n * 16, bit)
            norm(lambda span: x_v[span, :], bit * core + (own - bit) * h, n)

        lax.fori_loop(0, own // 16, norm_own, None)
        for copy in load_turns:
            copy.wait()
        low = lax.broadcasted_iota(jnp.int32, (rows + own, HEAD), 1) < HEAD // 2
        here = turn_v[...]
        there = pltpu.roll(here, HEAD // 2, 1)
        cos_v[...] = jnp.where(low, here, there)
        sin_v[...] = jnp.where(low, -there, here)
        shares = [pltpu.make_async_remote_copy(a_v.at[part_of(core, h)], a_v.at[part_of(core, h)], pair_send.at[h], pair_recv.at[h],
                                               device_id=partner, device_id_type=MESH) for h in range(2)]
        for copy in shares:
            copy.start()
        for copy in shares:
            copy.wait()

        def tile(i, high, low, store):
            slot = lax.rem(i, 3)
            t = lax.rem(lax.div(i, SIDE), 3)
            pltpu.make_async_copy(wq.at[:, pl.ds(0, TILE)], slots.at[slot], slot_sem.at[slot]).wait()

            @pl.when(i + 2 < 3 * phase)
            def _():
                fetch(i + 2)

            got = _dot(a_v[low:high, :], slots[slot], 1, 0).astype(jnp.bfloat16)
            for h in range(TILE // HEAD):
                cols = slice(h * HEAD, (h + 1) * HEAD)

                @pl.when(t < 2)
                def _():
                    wide = got[:, cols].astype(jnp.float32)
                    turned = wide * cos_v[low:high, :] + pltpu.roll(wide, HEAD // 2, 1) * sin_v[low:high, :]
                    store(turned.astype(jnp.bfloat16), cols)

                @pl.when(t == 2)
                def _():
                    store(got[:, cols], cols)

        def within(n, start, low, high, here, which):
            def step(r, _):
                g, o = lax.div(r, SIDE), lax.rem(r, SIDE)
                m = g * (SIDE - 1) + o

                def store(value, cols):
                    @pl.when(o < SIDE - 1)
                    def _():
                        lend[m, low:high, cols] = value

                    @pl.when(o == SIDE - 1)
                    def _():
                        recv[g, here, cols] = value

                tile(start + r, high, low, store)
                if which == 1:

                    @pl.when((r >= LATER) & (r < LATER + phase // 2))
                    def _():
                        cross_copy(phase // 2 + r - LATER).start()

                @pl.when(o > 0)
                def _():
                    own_copies(m - 1)[which].start()

            lax.fori_loop(0, n, step, None)

        within(phase, 0, 0, rows, block(chip), 0)

        passing = pltpu.make_async_remote_copy(a_v.at[borrowed(core)], a_v.at[borrowed(core)], pass_send, pass_recv,
                                               device_id=partner, device_id_type=MESH)

        def cross(r, _):
            def store(value, cols):
                send[r, :, cols] = value

            tile(phase + r, rows, own, store)

            @pl.when(r == phase // 2)
            def _():
                lending.wait_recv()

                def send_cross(n, _):
                    cross_copy(n).start()

                lax.fori_loop(0, phase // 2, send_cross, None)

                def norm_loan(n, _):
                    norm(lambda span: loan_v[span, :], rows + bit * core, n)

                lax.fori_loop(0, bit // 16, norm_loan, None)

            @pl.when(r == phase // 2 + 1)
            def _():
                passing.start()

        lax.fori_loop(0, phase, cross, None)
        passing.wait()
        lending.wait_send()
        within(phase, 2 * phase, rows, rows + own, first(counter), 1)

    pl.run_scoped(project, pltpu.VMEM((3, d, TILE), jnp.bfloat16), pltpu.SemaphoreType.DMA((3,)))

    def give_copy(w, s, o):
        c = chip_of(lax.rem(side + 1 + s, 2), near(o))
        return pltpu.make_async_remote_copy(osend.at[w, block(c)], orecv.at[w, lax.rem(1 + s, 2), place], o_send.at[w, s, o],
                                            o_recv.at[w, lax.rem(1 + s, 2), place], device_id=at(c), device_id_type=MESH)

    def finish(slots, acc, slot_sem):
        parts, wide = acc.shape[0], acc.shape[2]
        chunks = waves * 2 * parts

        def fetch(n):
            w, far, p = lax.rem(lax.div(n, parts), waves), lax.div(n, waves * parts), lax.rem(n, parts)
            slot = lax.rem(n, 3)
            across = pl.ds(pl.multiple_of(p * wide, wide), wide)

            def source(m, _):
                row = pl.multiple_of(half * core + (w * CHIPS + chip_of(lax.rem(side + far, 2), m)) * TILE, TILE)
                into = pl.ds(pl.multiple_of(m * TILE, TILE), TILE)
                pltpu.make_async_copy(wo.at[pl.ds(row, TILE), across], slots.at[slot, into], slot_sem.at[slot]).start()

            lax.fori_loop(0, SIDE, source, None)

        fetch(jnp.int32(0))
        fetch(jnp.int32(1))

        strip = 512

        def position(axis):
            r = lax.broadcasted_iota(jnp.int32, (strip, strip), axis)
            c, h, k = lax.div(r, rows), lax.rem(lax.div(r, own), 2), lax.rem(lax.div(r, bit), 2)
            return c * rows + k * own + h * bit + lax.rem(r, bit)

        hidden = position(0) > position(1)
        e = HEAD**-0.5 * LOG2E

        def give(w):
            def one(n, _):
                give_copy(w, lax.div(n, SIDE), lax.rem(n, SIDE)).start()

            lax.fori_loop(0, CHIPS - 1, one, None)

        def attend(w, _):
            def arrived(n, _):
                g, o = 3 * w + lax.div(n, SIDE), lax.rem(n, SIDE)
                m = near(o)

                @pl.when(o < SIDE - 1)
                def _():
                    c = chip_of(side, m)
                    pltpu.make_async_remote_copy(lend.at[0, pl.ds(0, rows)], recv.at[g, block(c)], l_send.at[0, 0], q_recv.at[g, m, 0],
                                                 device_id=at(c), device_id_type=MESH).wait_recv()
                    pltpu.make_async_remote_copy(lend.at[0, pl.ds(rows, own)], recv.at[g, first(chip_of(1 - side, m))], l_send.at[0, 1],
                                                 q_recv.at[g, m, 1], device_id=at(c), device_id_type=MESH).wait_recv()

                c = chip_of(1 - side, m)
                pltpu.make_async_remote_copy(send.at[0], recv.at[g, second(c)], c_send.at[0], q_recv.at[g, m, 2],
                                             device_id=at(c), device_id_type=MESH).wait_recv()

            lax.fori_loop(0, 3 * SIDE, arrived, None)

            @pl.when(w > 0)
            def _():
                give(w - 1)

            for h in range(2):
                vt_s[h, :HEAD, :] = recv[3 * w + 2, :, h * HEAD : (h + 1) * HEAD].T
                vt_s[h, HEAD:, :] = jnp.ones((16, tokens), jnp.bfloat16)
            for i in range(tokens // strip):

                def head(h, _):
                    lanes = pl.ds(pl.multiple_of(h * HEAD, HEAD), HEAD)
                    q = recv[3 * w, i * strip : (i + 1) * strip, lanes]
                    scores = [_dot(recv[3 * w + 1, b * strip : (b + 1) * strip, lanes], q, 1, 1) for b in range(i + 1)]
                    scores[i] = jnp.where(hidden, NEG, scores[i])
                    top = functools.reduce(jnp.maximum, [s.max(axis=0, keepdims=True) for s in scores])
                    mix = 0
                    for b, s in enumerate(scores):
                        weights = jnp.exp2((s - top) * e).astype(jnp.bfloat16)
                        mix = mix + _dot(vt_s[h, :, b * strip : (b + 1) * strip], weights, 1, 0)
                    seen = (mix[:HEAD] * (1 / mix[HEAD : HEAD + 1])).T.astype(jnp.bfloat16)
                    osend[w, i * strip : (i + 1) * strip, lanes] = seen

                lax.fori_loop(0, 2, head, None)
            orecv[w, 0, place] = osend[w, block(chip)]

        lax.fori_loop(0, waves, attend, None)
        give(waves - 1)

        def hand(p):
            return [pltpu.make_async_remote_copy(acc.at[p, part_of(other, h)], part.at[p, pl.ds(bit * h, bit)], p_send.at[p, h],
                                                 p_recv.at[p, h], device_id=partner, device_id_type=MESH) for h in range(2)]

        def chunk(n, _):
            w, far, p = lax.rem(lax.div(n, parts), waves), lax.div(n, waves * parts), lax.rem(n, parts)
            slot = lax.rem(n, 3)

            @pl.when(n + 2 < chunks)
            def _():
                fetch(n + 2)

            @pl.when(p == 0)
            def _():
                def arrived(m, _):
                    c = chip_of(lax.rem(side + far, 2), m)

                    @pl.when(c != chip)
                    def _():
                        pltpu.make_async_remote_copy(osend.at[w, block(c)], orecv.at[w, far, m], o_send.at[w, 0, 0],
                                                     o_recv.at[w, far, m], device_id=at(c), device_id_type=MESH).wait_recv()

                lax.fori_loop(0, SIDE, arrived, None)

            pltpu.make_async_copy(wo.at[pl.ds(0, SIDE * TILE), pl.ds(0, wide)], slots.at[slot], slot_sem.at[slot]).wait()
            seen = jnp.concatenate([orecv[w, far, m] for m in range(SIDE)], axis=1)
            more = _dot(seen, slots[slot], 1, 0)

            @pl.when(n < parts)
            def _():
                acc[p] = more

            @pl.when(n >= parts)
            def _():
                acc[p] += more

            @pl.when(n > chunks - parts)
            def _():
                for copy in hand(p - 1):
                    copy.start()

        lax.fori_loop(0, chunks, chunk, None)

        def sent(r, _):
            cross_copy(r).wait_send()

        def lent_out(n, _):
            for copy in own_copies(n):
                copy.wait_send()

        lax.fori_loop(0, phase, sent, None)
        lax.fori_loop(0, groups * (SIDE - 1), lent_out, None)
        for copy in hand(parts - 1):
            copy.start()

        def given(n, _):
            w, r = lax.div(n, CHIPS - 1), lax.rem(n, CHIPS - 1)
            give_copy(w, lax.div(r, SIDE), lax.rem(r, SIDE)).wait_send()

        lax.fori_loop(0, waves * (CHIPS - 1), given, None)

        def add(p, _):
            across = pl.ds(pl.multiple_of(p * wide, wide), wide)
            for h, copy in enumerate(hand(p)):
                copy.wait_recv()
                span = slice(bit * h, bit * (h + 1))
                total = acc[p, part_of(core, h), :] + part[p, span]
                y_ref[span, across] = (x_v[span, across].astype(jnp.float32) + total).astype(jnp.bfloat16)
                copy.wait_send()

        lax.fori_loop(0, parts, add, None)

    pieces = part.shape[0]
    pl.run_scoped(finish, pltpu.VMEM((3, SIDE * TILE, d // pieces), jnp.bfloat16), pltpu.VMEM((pieces, rows, d // pieces), jnp.float32),
                  pltpu.SemaphoreType.DMA((3,)))


def _turns(tokens):
    half = HEAD // 2
    angle = np.arange(tokens, dtype=np.float32)[:, None] * np.float32(THETA) ** (-np.arange(half, dtype=np.float32) / np.float32(half))
    angle = angle.astype(np.float32).astype(np.float64)
    return np.concatenate([np.cos(angle), np.sin(angle)], 1).astype(np.float32)


def solution(mesh):
    def step(x, gain, wq, wk, wv, wo):
        own, d = x.shape
        rows, tokens = 2 * own, 2 * own * CHIPS
        waves = wq.shape[1] // (2 * CHIPS * TILE)
        groups, pieces = 3 * waves, 4
        hbm, vmem = pl.BlockSpec(memory_space=pl.ANY), pl.BlockSpec(memory_space=pltpu.VMEM)
        dma, low, f32 = pltpu.SemaphoreType.DMA, jnp.bfloat16, jnp.float32
        return pl.pallas_call(
            _kernel,
            out_shape=jax.ShapeDtypeStruct((own, d), low),
            in_specs=[hbm, vmem, hbm, hbm, hbm, hbm, hbm],
            out_specs=vmem,
            scratch_shapes=[
                pltpu.VMEM((rows + own, d), low),
                pltpu.VMEM((own, d), low),
                pltpu.VMEM((1, d), f32),
                pltpu.VMEM((own // 2, d), low),
                pltpu.VMEM((rows + own, HEAD), f32),
                pltpu.VMEM((rows + own, HEAD), f32),
                pltpu.VMEM((rows + own, HEAD), f32),
                pltpu.VMEM((groups * SIDE, own, TILE), low),
                pltpu.VMEM((groups * (SIDE - 1), rows + own, TILE), low),
                pltpu.VMEM((groups, tokens, TILE), low),
                pltpu.VMEM((waves, tokens, TILE), low),
                pltpu.VMEM((waves, 2, SIDE, rows, TILE), low),
                pltpu.VMEM((pieces, own, d // pieces), f32),
                pltpu.VMEM((2, HEAD + 16, tokens), low),
                dma((7,)),
                dma((2,)),
                dma((2,)),
                dma,
                dma,
                dma,
                dma,
                dma((groups * SIDE,)),
                dma((groups * (SIDE - 1), 2)),
                dma((groups, SIDE, 3)),
                dma((waves, 2, SIDE)),
                dma((waves, 2, SIDE)),
                dma((pieces, 2)),
                dma((pieces, 2)),
            ],
            compiler_params=pltpu.CompilerParams(collective_id=0, has_side_effects=True, vmem_limit_bytes=67043328),
        )(x, gain, _turns(tokens), wq, wk, wv, wo)

    rows, whole = P(("dp", "sp"), None), P(None, None)
    return jax.shard_map(
        step,
        mesh=mesh,
        in_specs=(rows, P(None), whole, whole, whole, whole),
        out_specs=rows,
        check_vma=False,
    )
```
